32 devices in a mesh: rep: 8 (over y, x, core), tp: 4 (over z).
Axes of the slice: x: 2, y: 2, z: 4, core: 2. Of those that a mesh axis runs over, the one named last changes fastest.
Arguments:
- residual_in: bfloat16 [8, 512, 8192], P('rep', 'tp'), may hold values from -6 to 6
- norm_gain: bfloat16 [8192], replicated, may hold values from 0.099609375 to 1.8984375
- w_query: bfloat16 [8192, 4096], P(None, 'tp'), may hold values from -1 to 1
- w_keyval: bfloat16 [8192, 1024], P(None, 'tp'), may hold values from -0.0625 to 0.0625
- w_out: bfloat16 [4096, 8192], P('tp'), may hold values from -0.375 to 0.375
- score_head: bfloat16 [8192], replicated, may hold values from -0.0625 to 0.0625
- lengths: int32 [8], P('rep'), may hold values from 256 to 512
- policy_slots: bfloat16 [8, 768, 8192], P('rep', None, 'tp'), may hold values from -6 to 6
Outputs:
- scored_hidden: bfloat16 [8, 512, 8192], P('rep', 'tp')
- rewards: float32 [8], P('rep')
- policy_copies: bfloat16 [8, 768, 8192], P('rep', None, 'tp')
The draws below stay inside these ranges and needn't reach their ends.
All inputs are finite; a program needn't handle non-finite values.
Results may differ from the reference program's by a relative error of at most 0.017.
The reference program's roundings to bfloat16 on the way count: a program that leaves them out, or rounds other values in their place, can miss the bound.
Values may be sent and summed in bfloat16 or wider, within the bound.
A program may use at most 128 MiB of HBM per device.

```python
import jax
import jax.numpy as jnp
from jax import lax

D = 8192
QH = 32
KVH = 4
HS = 128
LEN = 512
PROWS = 768
QW = 4096
KW = 512
REPLICAS = 8
N_TP = 4


def draw_w_query(key, part):
    values = jax.random.normal(jax.random.fold_in(key, 11), (D, QW), jnp.float32) * D ** (-0.5)
    return jnp.clip(values, -1.0, 1.0).astype(jnp.bfloat16)


def with_ends(result, own_key, low, largest):
    longest = result.shape.index(max(result.shape))
    spots = []
    for shift in (0, 1):
        where = [jax.random.randint(jax.random.fold_in(own_key, axis), (), 0, length) for axis, length in enumerate(result.shape)]
        where[longest] = (where[longest] + shift) % result.shape[longest]
        spots.append(tuple(where))
    return result.at[spots[0]].set(low).at[spots[1]].set(largest)


def block_levels(rng, dims, pieces, least, largest):
    gain, own = 1.0, jax.random.fold_in(rng, 6)
    for position, blocks in pieces:
        draws = jnp.exp(jax.random.uniform(jax.random.fold_in(own, position), (blocks,), jnp.float32, least / len(pieces), largest / len(pieces)))
        gain = gain * jnp.repeat(draws, dims[position] // blocks).reshape([-1 if axis == position else 1 for axis in range(len(dims))])
    return gain


def centred(rng, dims, deviation, bound, cuts=(), held_as=jnp.bfloat16):
    result = jax.random.normal(rng, dims, jnp.float32) * deviation
    if len(cuts) > 0:
        result = block_levels(rng, dims, cuts, -0.22, 0.18) * result
    return jnp.clip(result, min=-bound, max=bound).astype(held_as)


def setup_inputs(seed: int = 0) -> dict:
    arg_keys = jax.random.split(jax.random.key(seed), 9)
    residual_in = centred(arg_keys[0], (REPLICAS, LEN, D), 1.0, 6.0, ((0, 8), (1, 4)))
    norm_gain = jnp.clip(1.0 + 0.18 * jax.random.normal(arg_keys[1], (D,), jnp.float32), 0.099609375, 1.8984375).astype(jnp.bfloat16)
    w_query = draw_w_query(jax.random.fold_in(arg_keys[8], 71), 0)
    w_keyval = centred(arg_keys[3], (D, 2 * KW), D ** -0.5, 0.0625, ((1, 4),))
    w_out = centred(arg_keys[4], (QW, D), (QW // 16) ** -0.5, 0.375, ((0, 4),))
    score_head = centred(arg_keys[5], (D,), D ** -0.5, 0.0625)
    lengths = with_ends(jax.random.randint(arg_keys[6], (REPLICAS,), LEN // 2, LEN + 1), jax.random.fold_in(arg_keys[6], 1), LEN // 2, LEN).astype(jnp.int32)
    policy_slots = centred(arg_keys[7], (REPLICAS, PROWS, D), 1.0, 6.0, ((0, 8), (2, 4)))
    return dict(residual_in=residual_in, norm_gain=norm_gain, w_query=w_query, w_keyval=w_keyval, w_out=w_out, score_head=score_head, lengths=lengths, policy_slots=policy_slots)


def one_rollout(residual_row, length, norm_gain, w_query, w_keyval, w_out, score_head):
    resid = residual_row.astype(jnp.float32)
    meansq = lax.optimization_barrier(jnp.mean(resid * resid, axis=-1, keepdims=True))
    normed = (resid * lax.rsqrt(meansq + 1e-05) * norm_gain.astype(jnp.float32)).astype(jnp.bfloat16)
    queries = jnp.dot(normed, w_query, preferred_element_type=jnp.float32).astype(jnp.bfloat16)
    keyvals = jnp.dot(normed, w_keyval, preferred_element_type=jnp.float32).astype(jnp.bfloat16)
    group = QH // KVH
    qheads = queries.reshape(LEN, QH, HS).transpose(1, 0, 2).astype(jnp.float32)
    kheads = keyvals[:, :KW].reshape(LEN, KVH, HS).transpose(1, 0, 2)
    vheads = keyvals[:, KW:].reshape(LEN, KVH, HS).transpose(1, 0, 2)
    kheads = jnp.repeat(kheads, group, axis=0).astype(jnp.float32)
    vheads = jnp.repeat(vheads, group, axis=0).astype(jnp.float32)
    scores = jnp.einsum('hqd,hkd->hqk', qheads, kheads) * HS ** (-0.5)
    rowpos = jnp.arange(LEN, dtype=jnp.int32)[:, None]
    colpos = jnp.arange(LEN, dtype=jnp.int32)[None, :]
    valid = (colpos <= rowpos) & (colpos < length)
    scores = jnp.where(valid[None], scores, -1e+30)
    probs = jax.nn.softmax(scores, axis=-1).astype(jnp.bfloat16)
    attended = jnp.einsum('hqk,hkd->hqd', probs.astype(jnp.float32), vheads).astype(jnp.bfloat16)
    attended = attended.transpose(1, 0, 2).reshape(LEN, QW)
    groups = attended.reshape(LEN, N_TP, QW // N_TP).astype(jnp.float32)
    wgroups = w_out.reshape(N_TP, QW // N_TP, D).astype(jnp.float32)
    partial_value = jnp.einsum('lti,tid->tld', groups, wgroups).astype(jnp.bfloat16)
    partial_value = lax.optimization_barrier(partial_value)
    summed = lax.optimization_barrier(jnp.sum(partial_value.astype(jnp.float32), axis=0))
    hidden = (resid + summed).astype(jnp.bfloat16)
    head = score_head.astype(jnp.float32)
    last_row = lax.dynamic_slice_in_dim(hidden, (length - 1).astype(jnp.int32), 1, 0)[0]
    reward = jnp.sum(last_row.astype(jnp.float32) * head)
    pooled = jnp.sum(hidden.astype(jnp.float32) * head[None, :]) * LEN ** (-0.5)
    return (hidden, reward + pooled)

def reference(residual_in, norm_gain, w_query, w_keyval, w_out, score_head, lengths, policy_slots):

    def step(pair):
        return one_rollout(pair[0], pair[1], norm_gain, w_query, w_keyval, w_out, score_head)
    scored_hidden, rewards = lax.map(step, (residual_in, lengths.astype(jnp.int32)))
    policy_copies = jnp.broadcast_to(policy_slots[0:1], policy_slots.shape)
    return (scored_hidden, rewards.astype(jnp.float32), policy_copies)
```

```python
import functools

import jax
import jax.numpy as jnp
from jax import lax
from jax.experimental import pallas as pl
from jax.experimental.pallas import tpu as pltpu
from jax.sharding import PartitionSpec as P

QH = 32
KVH = 4
HS = 128
MESH = pl.DeviceIdType.MESH
F32 = jnp.float32
BF16 = jnp.bfloat16
CHUNKS = 8
DEPTH = 3
GO_STEP = 8
GO_LAST = 44
LAG = 2
NEVER = 1 << 20
POL_TICKS = (24, 56)

TUNED = {(4, 8): {(0, 0): dict(up={0: 0}, down={1: 4, 2: 20, 3: 47}, sum_up={1: 31, 2: 47, 3: 74}, sum_down={}, attend={0: 30, 1: 31, 2: 36, 3: 54}, own=1, fin=91), (0, 1): dict(up={0: 22}, down={1: 31, 2: 39, 3: 63}, sum_up={1: 59, 2: 71, 3: 94}, sum_down={}, attend={0: 45, 1: 59, 2: 67, 3: 74}, own=10, fin=97), (1, 0): dict(up={0: 1, 1: 9}, down={1: 0, 2: 9, 3: 21}, sum_up={2: 43, 3: 81}, sum_down={0: 84}, attend={0: 15, 1: 30, 2: 39, 3: 48}, own=14, fin=95), (1, 1): dict(up={0: 21, 1: 29}, down={1: 20, 2: 30, 3: 38}, sum_up={2: 73, 3: 91}, sum_down={0: 71}, attend={0: 37, 1: 41, 2: 70, 3: 80}, own=13, fin=115), (2, 0): dict(up={0: 5, 1: 13, 2: 32}, down={2: 0, 3: 10}, sum_up={3: 72}, sum_down={0: 27, 1: 72}, attend={0: 14, 1: 45, 2: 46, 3: 48}, own=3, fin=65), (2, 1): dict(up={0: 19, 1: 27, 2: 42}, down={2: 20, 3: 28}, sum_up={3: 85}, sum_down={0: 49, 1: 84}, attend={0: 28, 1: 53, 2: 65, 3: 67}, own=6, fin=84), (3, 0): dict(up={0: 6, 1: 18, 2: 31}, down={3: 3}, sum_up={}, sum_down={0: 19, 1: 29, 2: 78}, attend={0: 18, 1: 27, 2: 42, 3: 46}, own=17, fin=112), (3, 1): dict(up={0: 2, 1: 31, 2: 44}, down={3: 0}, sum_up={}, sum_down={0: 28, 1: 60, 2: 72}, attend={0: 24, 1: 49, 2: 60, 3: 76}, own=3, fin=114), }}


def plan(n, C):
    if (n, C) in TUNED:
        return TUNED[(n, C)]
    table = {}
    pad = LAG * (n - 1) + 3
    for t in range(n):
        w = n - 1 - t
        for p in range(2):
            late = p * n * C
            up = {j: late + j * C + LAG * t for j in range(t + 1) if j < n - 1}
            down = {b: late + (b - t) * C + LAG * w for b in range(t, n) if b > 0}
            attend = {b: late + min(b + 1, n - 1) * C + pad + b for b in range(n)}
            sums = late + (n - 1) * C + pad + n
            sum_up = {b: sums + (b - 1) * C + 2 * t for b in range(t + 1, n)}
            sum_down = {b: sums + b * C + 2 * w for b in range(t)}
            table[t, p] = dict(
                up=up, down=down, sum_up=sum_up, sum_down=sum_down, attend=attend,
                own=late + 1, fin=sums + (n - 1) * C + 2 * n,
            )
    return table


def kernel(
    n, R, kvw, heads,
    resid_h, gain, wq_h, wkv_h, wo_h, head, lens, pol_in,
    out_h, rew, pol_out,
    wq, wkv, wo, resid, nrm, part, accq, acckv, kvown, kvin, kf, vf, att, score, rmy, rin,
    load_sem, ag_send, ag_recv, rs_send, rs_recv, kv_send, kv_recv, r_send, r_recv, p_send, p_recv, p_loc, out_sem, go_sem,
):
    t = lax.axis_index("tp")
    r = lax.axis_index("rep")
    par = lax.rem(r, 2)
    C = nrm.shape[1]
    rows, cols = nrm.shape[2], nrm.shape[3]
    seq = n * rows
    length = lens[0]

    def chunk_of(ref, c):
        return ref.at[:, pl.ds(pl.multiple_of(c * cols, cols), cols)]

    loads = [pltpu.make_async_copy(chunk_of(resid_h.at[0], c), resid.at[c], load_sem.at[c]) for c in range(C)]
    wloads = [
        pltpu.make_async_copy(wkv_h, wkv, load_sem.at[C + 1]),
        pltpu.make_async_copy(wq_h, wq, load_sem.at[C]),
    ]
    oloads = [pltpu.make_async_copy(chunk_of(wo_h, c), wo.at[c], load_sem.at[C + 2 + c]) for c in range(C)]
    for cp in loads:
        cp.start()

    barrier = pltpu.get_barrier_semaphore()
    for k in range(1, n):
        pl.semaphore_signal(barrier, inc=1, device_id={"tp": lax.rem(t + k, n)}, device_id_type=MESH)
    for k in range(1, R):
        pl.semaphore_signal(barrier, inc=1, device_id={"rep": lax.rem(r + k, R)}, device_id_type=MESH)

    for cp in loads:
        cp.wait()
    for cp in wloads + oloads:
        cp.start()

    def sq(c, acc):
        x = resid[c].astype(F32)
        return acc + jnp.sum(x * x, axis=1, keepdims=True)

    ms = lax.fori_loop(0, C, sq, jnp.zeros((rows, 1), F32))
    scale = lax.rsqrt(ms / (C * cols) + 1e-05)

    def norm(c, carry):
        nrm[t, c] = (resid[c].astype(F32) * scale * gain[c].astype(F32)).astype(BF16)
        return carry

    lax.fori_loop(0, C, norm, 0)
    pl.semaphore_wait(barrier, n - 1 + R - 1)

    steps = R.bit_length() - 1

    def pol(src, s):
        return pltpu.make_async_remote_copy(
            src, pol_out, p_send.at[s], p_recv, device_id={"rep": r + (R >> (s + 1))}, device_id_type=MESH
        )

    @pl.when(r == 0)
    def _():
        for s in range(steps):
            pol(pol_in, s).start()
        pltpu.make_async_copy(pol_in, pol_out, p_loc).start()

    def pol_point(s):
        gap = R >> (s + 1)

        @pl.when(lax.rem(r, 2 * gap) == gap)
        def _():
            pltpu.make_async_copy(pol_out, pol_out, p_recv).wait()
            for q in range(s + 1, steps):
                pol(pol_out, q).start()

    table = plan(n, C)
    last = 0
    for entry in table.values():
        last = max(last, entry["fin"] + C, GO_LAST + 1)

    def pick(value):
        out = jnp.int32(value(table[0, 0]))
        for (a, p), entry in table.items():
            out = jnp.where((t == a) & (par == p), jnp.int32(value(entry)), out)
        return out

    def starts(name, low, high):
        result = []
        for b in range(n):
            def value(entry, b=b):
                known = entry[name]
                if b in known:
                    return known[b]
                return low if known and b < min(known) else high
            result.append(pick(value))
        return result

    up_at = starts("up", -NEVER, NEVER)
    down_at = starts("down", -NEVER, NEVER)
    sum_up_at = starts("sum_up", -NEVER, NEVER)
    sum_down_at = starts("sum_down", -NEVER, NEVER)
    attend_at = starts("attend", -NEVER, NEVER)
    own_at = pick(lambda e: e["own"])
    fin_at = pick(lambda e: e["fin"])

    def first_mm(e, a):
        return min([e["own"]] + [v for name in ("up", "down") for b, v in e[name].items() if b != a])

    mm_at = jnp.int32(0)
    wo_at = jnp.int32(0)
    for (a, p), e in table.items():
        here = (t == a) & (par == p)
        mm_at = jnp.where(here, jnp.int32(first_mm(e, a)), mm_at)
        wo_at = jnp.where(here, jnp.int32(min([e["fin"]] + list(e["sum_up"].values()) + list(e["sum_down"].values()))), wo_at)

    def at_tick(k, begins):
        j = jnp.int32(-1)
        begin = jnp.int32(NEVER)
        for b in range(n):
            hit = k >= begins[b]
            j = jnp.where(hit, b, j)
            begin = jnp.where(hit, begins[b], begin)
        c = k - begin
        live = (c >= 0) & (c < C)
        return live, jnp.maximum(j, 0), jnp.clip(c, 0, C - 1)

    group = QH // KVH
    pieces = kvw // HS
    my_head = (t * heads) // group

    def kv_copy(b, p, k):
        target = lax.rem(t + k, n)
        gid = t * pieces + p
        is_v = gid // KVH
        return target, gid, pltpu.make_async_remote_copy(
            kvown.at[b, p], kvin.at[b, is_v], kv_send.at[b, p, k - 1], kv_recv.at[b, is_v],
            device_id={"tp": target}, device_id_type=MESH,
        )

    def multiply(b, c):
        x = nrm[b, c]
        acckv[b] += jnp.dot(x, wkv[c], preferred_element_type=F32)
        accq[b] += jnp.dot(x, wq[c], preferred_element_type=F32)

        @pl.when(c == C - 1)
        def _():
            span = pl.ds(pl.multiple_of(b * rows, rows), rows)
            for p in range(pieces):
                kvown[b, p] = acckv[b, :, p * HS : (p + 1) * HS].astype(BF16)
            for p in range(pieces):
                for k in range(1, n):
                    target, gid, cp = kv_copy(b, p, k)

                    @pl.when(lax.rem(gid, KVH) == (target * heads) // group)
                    def _(cp=cp):
                        cp.start()

                gid = t * pieces + p
                here = lax.rem(gid, KVH) == my_head

                @pl.when(here & (gid < KVH))
                def _(p=p):
                    kf[span, :] = kvown[b, p]

                @pl.when(here & (gid >= KVH))
                def _(p=p):
                    vf[span, :] = kvown[b, p]

    def ag_copy(d, b, c, slot):
        return pltpu.make_async_remote_copy(
            nrm.at[b, c], nrm.at[b, c], ag_send.at[d, slot], ag_recv.at[b, c],
            device_id={"tp": t + (1 if d == 0 else -1)}, device_id_type=MESH,
        )

    def ag_step(d, k):
        live, b, c = at_tick(k, up_at if d == 0 else down_at)
        i = (b if d == 0 else b - t) * C + c
        has = (t < n - 1) if d == 0 else (t > 0)

        @pl.when(live & (b != t))
        def _():
            pltpu.make_async_copy(nrm.at[b, c], nrm.at[b, c], ag_recv.at[b, c]).wait()

        @pl.when(live & has)
        def _():
            @pl.when(i >= DEPTH)
            def _():
                ag_copy(d, b, c, lax.rem(i, DEPTH)).wait_send()

            ag_copy(d, b, c, lax.rem(i, DEPTH)).start()

        return live & (b != t), b, c

    def rs_copy(d, b, c, slot):
        dst = b if d == 0 else jnp.where(b == t - 1, n, b)
        return pltpu.make_async_remote_copy(
            part.at[b, c], part.at[dst, c], rs_send.at[d, slot], rs_recv.at[dst, c],
            device_id={"tp": t + (1 if d == 0 else -1)}, device_id_type=MESH,
        )

    def rs_wait(slot, c):
        pltpu.make_async_copy(part.at[slot, c], part.at[slot, c], rs_recv.at[slot, c]).wait()

    def project(b, c):
        return jnp.dot(att[b], wo[c], preferred_element_type=F32).astype(BF16)

    def rs_step(d, k):
        live, b, c = at_tick(k, sum_up_at if d == 0 else sum_down_at)
        i = (b - t - 1 if d == 0 else b) * C + c
        has = (t > 0) if d == 0 else (t < n - 1)

        @pl.when(live)
        def _():
            mine = project(b, c)

            @pl.when(has)
            def _():
                rs_wait(b, c)
                part[b, c] = (part[b, c].astype(F32) + mine.astype(F32)).astype(BF16)

            @pl.when(jnp.logical_not(has))
            def _():
                part[b, c] = mine

            @pl.when(i >= DEPTH)
            def _():
                rs_copy(d, b, c, lax.rem(i, DEPTH)).wait_send()

            rs_copy(d, b, c, lax.rem(i, DEPTH)).start()

    def attend(b):
        span = pl.ds(pl.multiple_of(b * rows, rows), rows)
        for is_v, full in ((0, kf), (1, vf)):
            owner = (is_v * KVH + my_head) // pieces

            @pl.when(owner != t)
            def _(is_v=is_v, full=full):
                pltpu.make_async_copy(kvin.at[b, is_v], kvin.at[b, is_v], kv_recv.at[b, is_v]).wait()
                full[span, :] = kvin[b, is_v]

        rowpos = b * rows + lax.broadcasted_iota(jnp.int32, (rows, seq), 0)
        colpos = lax.broadcasted_iota(jnp.int32, (rows, seq), 1)
        valid = (colpos <= rowpos) & (colpos < length)
        for h in range(heads):
            s = lax.dot_general(
                accq[b, :, h * HS : (h + 1) * HS].astype(BF16), kf[...],
                (((1,), (1,)), ((), ())), preferred_element_type=F32,
            ) * HS ** (-0.5)
            s = jnp.where(valid, s, -1e30)
            e = jnp.exp(s - jnp.max(s, axis=1, keepdims=True))
            pr = (e / jnp.sum(e, axis=1, keepdims=True)).astype(BF16)
            att[b, :, h * HS : (h + 1) * HS] = jnp.dot(
                pr, vf[...], preferred_element_type=F32
            ).astype(BF16)

    def fin(c):
        total = project(t, c).astype(F32)

        @pl.when(t > 0)
        def _():
            rs_wait(t, c)

        @pl.when(t < n - 1)
        def _():
            rs_wait(n, c)

        below = jnp.where(t > 0, part[t, c].astype(F32), 0.0)
        above = jnp.where(t < n - 1, part[n, c].astype(F32), 0.0)
        hid = (resid[c].astype(F32) + (total + below + above)).astype(BF16)
        resid[c] = hid
        pltpu.make_async_copy(resid.at[c], chunk_of(out_h.at[0], c), out_sem.at[c]).start()
        weighed = hid.astype(F32) * head[c].astype(F32)
        acc = score[...]
        for q in range(cols // HS):
            acc = acc + weighed[:, q * HS : (q + 1) * HS]
        score[...] = acc

    def zero():
        kf[...] = jnp.zeros_like(kf)
        vf[...] = jnp.zeros_like(vf)
        score[...] = jnp.zeros_like(score)
        for b in range(n):
            accq[b] = jnp.zeros(accq.shape[1:], F32)
            acckv[b] = jnp.zeros(acckv.shape[1:], F32)

    def tick(k, carry):
        @pl.when((lax.rem(k, GO_STEP) == 0) & (k > 0) & (k <= GO_LAST))
        def _():
            @pl.when(par == 0)
            def _():
                pl.semaphore_signal(go_sem, inc=1, device_id={"rep": r + 1}, device_id_type=MESH)

            @pl.when(par == 1)
            def _():
                pl.semaphore_wait(go_sem, 1)

        @pl.when(k == mm_at)
        def _():
            zero()
            for cp in wloads:
                cp.wait()

        @pl.when(k == wo_at)
        def _():
            for cp in oloads:
                cp.wait()

        for d in (0, 1):
            live, b, c = ag_step(d, k)

            @pl.when(live)
            def _(b=b, c=c):
                multiply(b, c)

        own = k - own_at

        @pl.when((own >= 0) & (own < C))
        def _():
            multiply(t, jnp.clip(own, 0, C - 1))

        due = jnp.int32(-1)
        for b in range(n):
            due = jnp.where(k == attend_at[b], b, due)

        @pl.when(due >= 0)
        def _():
            attend(jnp.maximum(due, 0))

        for s in range(steps - 1):
            @pl.when(k == POL_TICKS[min(s, len(POL_TICKS) - 1)] + s)
            def _(s=s):
                pol_point(s)

        rs_step(0, k)
        rs_step(1, k)
        f = k - fin_at

        @pl.when((f >= 0) & (f < C))
        def _():
            fin(jnp.clip(f, 0, C - 1))

        return carry

    lax.fori_loop(0, last, tick, 0)

    local_last = length - 1 - t * rows
    rowid = lax.broadcasted_iota(jnp.int32, (rows, 1), 0)
    weight = jnp.where(rowid == local_last, 1.0, 0.0) + seq ** (-0.5)
    rmy[...] = jnp.broadcast_to(jnp.sum(score[...] * weight, keepdims=True), rmy.shape)

    def rcopy(k):
        return pltpu.make_async_remote_copy(
            rmy, rin.at[k - 1], r_send.at[k - 1], r_recv.at[k - 1],
            device_id={"tp": lax.rem(t + k, n)}, device_id_type=MESH,
        )

    for k in range(1, n):
        rcopy(k).start()
    pol_point(steps - 1)

    for d in (0, 1):
        has = (t < n - 1) if d == 0 else (t > 0)

        @pl.when(has)
        def _(d=d):
            for q in range(DEPTH):
                ag_copy(d, t, 0, q).wait_send()
                rs_copy(d, t, 0, q).wait_send()

    def kv_drain(b, carry):
        for p in range(pieces):
            for k in range(1, n):
                target, gid, cp = kv_copy(b, p, k)

                @pl.when(lax.rem(gid, KVH) == (target * heads) // group)
                def _(cp=cp):
                    cp.wait_send()
        return carry

    lax.fori_loop(0, n, kv_drain, 0)

    total = rmy[...]
    for k in range(1, n):
        rcopy(k).wait()
        total = total + rin[k - 1]
    rew[...] = total
    for c in range(C):
        pltpu.make_async_copy(resid.at[c], chunk_of(out_h.at[0], c), out_sem.at[c]).wait()

    @pl.when(r == 0)
    def _():
        for s in range(steps):
            pol(pol_in, s).wait_send()
        pltpu.make_async_copy(pol_in, pol_out, p_loc).wait()

    for s in range(steps - 1):
        gap = R >> (s + 1)

        @pl.when(lax.rem(r, 2 * gap) == gap)
        def _(s=s):
            for q in range(s + 1, steps):
                pol(pol_out, q).wait_send()


def solution(mesh):
    n, R = mesh.shape["tp"], mesh.shape["rep"]

    def on_device(residual_in, norm_gain, w_query, w_keyval, w_out, score_head, lengths, policy_slots):
        rows, width = residual_in.shape[1:]
        qw, kvw = w_query.shape[1], w_keyval.shape[1]
        heads = qw // HS
        C = CHUNKS
        cols = width // C
        sem = pltpu.SemaphoreType.DMA
        vm = pl.BlockSpec(memory_space=pltpu.VMEM)
        hbm = pl.BlockSpec(memory_space=pl.ANY)
        hidden, reward, policy = pl.pallas_call(
            functools.partial(kernel, n, R, kvw, heads),
            out_shape=(
                jax.ShapeDtypeStruct(residual_in.shape, BF16),
                jax.ShapeDtypeStruct((8, 128), F32),
                jax.ShapeDtypeStruct(policy_slots.shape, BF16),
            ),
            in_specs=[hbm, vm, hbm, hbm, hbm, vm, pl.BlockSpec(memory_space=pltpu.SMEM), hbm],
            out_specs=(hbm, vm, hbm),
            scratch_shapes=[
                pltpu.VMEM((C, cols, qw), BF16),
                pltpu.VMEM((C, cols, kvw), BF16),
                pltpu.VMEM((C, qw, cols), BF16),
                pltpu.VMEM((C, rows, cols), BF16),
                pltpu.VMEM((n, C, rows, cols), BF16),
                pltpu.VMEM((n + 1, C, rows, cols), BF16),
                pltpu.VMEM((n, rows, qw), F32),
                pltpu.VMEM((n, rows, kvw), F32),
                pltpu.VMEM((n, kvw // HS, rows, HS), BF16),
                pltpu.VMEM((n, 2, rows, HS), BF16),
                pltpu.VMEM((n * rows, HS), BF16),
                pltpu.VMEM((n * rows, HS), BF16),
                pltpu.VMEM((n, rows, qw), BF16),
                pltpu.VMEM((rows, 128), F32),
                pltpu.VMEM((8, 128), F32),
                pltpu.VMEM((n - 1, 8, 128), F32),
                sem((2 * C + 2,)),
                sem((2, DEPTH)),
                sem((n, C)),
                sem((2, DEPTH)),
                sem((n + 1, C)),
                sem((n, kvw // HS, n - 1)),
                sem((n, 2)),
                sem((n - 1,)),
                sem((n - 1,)),
                sem((R.bit_length() - 1,)),
                sem,
                sem,
                sem((C,)),
                pltpu.SemaphoreType.REGULAR,
            ],
            compiler_params=pltpu.CompilerParams(
                collective_id=0, has_side_effects=True, vmem_limit_bytes=67043328
            ),
        )(
            residual_in,
            norm_gain.reshape(C, 1, cols),
            w_query.reshape(C, cols, qw),
            w_keyval.reshape(C, cols, kvw),
            w_out,
            score_head.reshape(C, 1, cols),
            lengths,
            policy_slots,
        )
        return hidden, reward[0, :1], policy

    return jax.shard_map(
        on_device,
        mesh=mesh,
        in_specs=(
            P("rep", "tp", None),
            P(),
            P(None, "tp"),
            P(None, "tp"),
            P("tp", None),
            P(),
            P("rep"),
            P("rep", None, "tp"),
        ),
        out_specs=(P("rep", "tp", None), P("rep"), P("rep", None, "tp")),
        check_vma=False,
    )
```

```python
import functools

import jax
import jax.numpy as jnp
from jax import lax
from jax.experimental import pallas as pl
from jax.experimental.pallas import tpu as pltpu
from jax.sharding import PartitionSpec as P

QH = 32
KVH = 4
HS = 128
MESH = pl.DeviceIdType.MESH
F32 = jnp.float32
BF16 = jnp.bfloat16
CHUNKS = 16
DEPTH = 2
LAG = 2
NEVER = 1 << 20
UP, DOWN, MM_UP, MM_DOWN, ATTEND, SUM_UP, SUM_DOWN, FIN, SPREAD, PAIR, POLICY = range(11)
NOTHING = 15
PER_WORD = 7
POLICY_OPS = 4

PREFIX = {(4, 16): [0, 1, 2, 0]}
TUNED = {(4, 16): {
    (0, 0): [2, 101, 1, 101, 3, 801, 101, 1, 101, 1, 101, 1, 101, 1, 101, 1, 901, 101, 1, 301, 101, 301, 1, 302, 101, 301, 1, 303, 1001, 1, 101, 401, 1, 101, 401, 101, 304, 101, 303, 102, 301, 401, 101, 401, 502, 101, 301, 101, 501, 101, 301, 501, 101, 501, 101, 301, 501, 101, 501, 101, 301, 501, 101, 501, 101, 301, 501, 101, 501, 101, 301, 501, 1001, 101, 501, 101, 301, 501, 101, 501, 101, 501, 301, 401, 101, 401, 101, 502, 301, 101, 501, 101, 301, 501, 101, 501, 101, 301, 501, 101, 501, 101, 301, 501, 101, 501, 101, 301, 501, 101, 501, 101, 301, 501, 101, 501, 101, 301, 501, 101, 501, 101, 501, 1001, 301, 402, 502, 703, 501, 701, 501, 701, 501, 701, 501, 701, 501, 1001, 701, 501, 701, 501, 701, 501, 701, 501, 701, 501, 701, 501, 701, 501, 701, 501, 701, 501],
    (0, 1): [2, 101, 1, 101, 3, 801, 101, 1, 101, 1, 101, 1, 101, 1, 101, 1, 901, 101, 1, 301, 101, 301, 1, 302, 101, 301, 1, 303, 1001, 1, 101, 401, 1, 101, 401, 101, 304, 101, 303, 102, 301, 401, 101, 401, 502, 101, 301, 501, 101, 501, 101, 301, 501, 101, 501, 101, 301, 501, 101, 501, 101, 301, 501, 101, 501, 101, 301, 501, 101, 501, 101, 301, 1001, 501, 101, 501, 101, 301, 501, 101, 501, 101, 301, 401, 101, 401, 502, 101, 301, 501, 101, 502, 101, 301, 501, 101, 501, 101, 301, 501, 101, 501, 101, 301, 501, 101, 501, 101, 301, 501, 101, 501, 101, 301, 501, 101, 501, 101, 301, 501, 102, 1001, 301, 402, 502, 702, 501, 701, 501, 701, 501, 701, 501, 701, 501, 701, 1001, 501, 701, 501, 701, 501, 701, 501, 701, 501, 701, 501, 701, 501, 701, 501, 701, 501, 701],
    (1, 0): [1, 104, 2, 801, 101, 1, 101, 1, 101, 1, 101, 1, 101, 1, 101, 1, 101, 1, 101, 1, 101, 1, 901, 101, 1, 101, 1, 206, 1001, 1, 201, 1, 102, 302, 1, 201, 101, 401, 1, 401, 1, 101, 301, 101, 302, 1, 302, 101, 301, 1, 401, 101, 401, 1, 101, 301, 1, 301, 101, 302, 1, 101, 1, 101, 301, 1, 101, 1, 101, 301, 1, 101, 1, 101, 301, 1, 101, 1, 101, 1001, 301, 401, 1, 101, 401, 101, 301, 102, 301, 102, 301, 101, 501, 101, 501, 301, 101, 501, 101, 501, 301, 101, 501, 101, 501, 301, 101, 501, 101, 501, 301, 101, 501, 101, 501, 301, 401, 501, 601, 401, 501, 602, 502, 601, 701, 501, 601, 501, 701, 601, 701, 501, 1001, 601, 701, 501, 601, 701, 501, 601, 701, 501, 601, 701, 501, 601, 701, 501, 601, 701, 501, 601, 1001, 701, 501, 601, 701, 501, 601, 701, 501, 601, 701, 501, 701, 501, 701, 501, 701, 503],
    (1, 1): [1, 104, 2, 801, 101, 1, 101, 1, 101, 1, 101, 1, 101, 1, 101, 1, 101, 1, 101, 1, 101, 1, 901, 101, 1, 101, 1, 202, 1, 101, 202, 1001, 202, 1, 101, 201, 101, 301, 1, 201, 101, 401, 1, 401, 1, 101, 301, 101, 302, 1, 302, 101, 301, 1, 301, 101, 401, 1, 401, 1, 101, 302, 101, 301, 1, 301, 101, 301, 1, 101, 1, 101, 301, 1, 101, 1, 101, 301, 1, 101, 1, 101, 301, 1001, 1, 401, 101, 401, 1, 101, 301, 102, 301, 102, 301, 502, 101, 501, 101, 301, 501, 101, 501, 101, 301, 501, 101, 501, 101, 301, 501, 101, 501, 101, 301, 501, 101, 501, 101, 301, 401, 501, 601, 401, 501, 601, 501, 601, 501, 601, 501, 601, 701, 601, 501, 701, 501, 1001, 601, 701, 501, 601, 701, 501, 601, 701, 501, 601, 701, 501, 601, 701, 501, 601, 701, 501, 601, 1001, 701, 501, 601, 701, 501, 601, 701, 501, 601, 701, 501, 701, 501, 701, 501, 701, 501, 701, 501],
    (2, 0): [2, 103, 801, 101, 1, 101, 1, 101, 1, 101, 1, 101, 1, 101, 1, 101, 1, 101, 1, 101, 901, 1, 101, 1, 101, 202, 1, 101, 203, 1, 101, 1001, 201, 302, 1, 301, 101, 303, 1, 101, 201, 302, 1, 101, 301, 101, 301, 2, 201, 401, 1, 101, 401, 1, 101, 201, 301, 101, 1, 201, 101, 301, 1, 101, 1, 201, 101, 301, 1, 101, 1, 201, 101, 301, 1, 101, 1, 201, 101, 301, 1, 101, 1001, 1, 201, 101, 301, 1, 601, 1, 201, 601, 1, 601, 1, 201, 401, 1, 601, 401, 1, 601, 401, 1, 601, 401, 1, 601, 401, 601, 1, 401, 601, 1, 601, 1, 601, 1, 601, 1, 601, 1, 601, 1, 601, 1, 601, 1, 601, 1, 607, 501, 601, 1001, 501, 601, 701, 501, 601, 701, 501, 601, 701, 501, 601, 701, 501, 601, 701, 501, 601, 701, 501, 1001, 601, 701, 501, 701, 501, 701, 501, 701, 501, 701, 501, 701, 502, 701, 501, 703],
    (2, 1): [2, 103, 801, 101, 1, 101, 1, 101, 1, 101, 1, 101, 1, 101, 1, 101, 1, 101, 1, 101, 901, 1, 101, 1, 101, 202, 1, 101, 203, 1, 101, 1001, 201, 302, 1, 301, 101, 302, 1, 201, 101, 302, 1, 301, 101, 301, 1, 201, 101, 1, 401, 1, 401, 101, 1, 201, 101, 302, 1, 201, 101, 1, 101, 301, 1, 201, 101, 1, 101, 301, 1, 201, 101, 1, 101, 301, 1, 201, 101, 1, 101, 301, 1, 1001, 201, 101, 1, 101, 301, 1, 201, 601, 1, 601, 1, 201, 601, 401, 1, 601, 401, 1, 601, 401, 1, 401, 1, 601, 401, 601, 1, 401, 601, 1, 601, 1, 601, 1, 601, 1, 601, 1, 601, 1, 601, 1, 601, 1, 601, 1, 606, 501, 601, 501, 601, 1001, 501, 701, 601, 501, 701, 601, 501, 701, 601, 501, 701, 601, 501, 701, 601, 501, 701, 601, 501, 1001, 701, 601, 501, 701, 601, 501, 701, 501, 701, 501, 701, 501, 701, 501, 701, 501, 703],
    (3, 0): [106, 801, 102, 1, 101, 1, 101, 1, 101, 901, 1, 101, 201, 1, 201, 101, 302, 1, 201, 101, 302, 1, 301, 101, 302, 1001, 301, 1, 101, 201, 2, 201, 2, 201, 2, 201, 2, 201, 401, 1, 401, 602, 1, 201, 1, 601, 1, 201, 601, 1, 601, 1, 201, 601, 1, 601, 1, 201, 601, 1, 601, 1, 201, 601, 1, 601, 1, 201, 601, 1, 601, 1001, 1, 201, 601, 1, 601, 3, 601, 201, 401, 1, 401, 602, 1, 202, 1, 601, 1, 201, 601, 1, 601, 1, 201, 601, 1, 601, 1, 201, 601, 1, 601, 1, 201, 601, 1, 601, 1, 201, 601, 1, 601, 1, 201, 401, 601, 401, 601, 1001, 401, 601, 401, 603, 701, 601, 701, 602, 701, 601, 701, 601, 701, 601, 1001, 701, 601, 701, 601, 701, 601, 701, 601, 701, 601, 701, 601, 701, 601, 704],
    (3, 1): [106, 801, 102, 1, 101, 1, 101, 1, 101, 901, 1, 101, 301, 1, 301, 101, 302, 1, 301, 101, 302, 1, 301, 101, 202, 1001, 1, 201, 101, 201, 2, 201, 2, 201, 2, 201, 2, 201, 401, 1, 401, 601, 1, 601, 201, 601, 1, 601, 1, 201, 601, 1, 601, 1, 201, 601, 1, 601, 1, 201, 601, 1, 601, 1, 201, 601, 1, 601, 1, 201, 601, 1, 1001, 601, 1, 201, 601, 1, 601, 3, 201, 401, 1, 401, 1, 602, 202, 1, 602, 1, 201, 601, 1, 601, 1, 201, 601, 1, 601, 1, 201, 601, 1, 601, 1, 201, 601, 1, 601, 1, 201, 601, 1, 601, 1, 201, 401, 601, 401, 1001, 601, 401, 601, 401, 602, 701, 601, 701, 601, 701, 601, 701, 601, 701, 601, 701, 1001, 601, 701, 601, 701, 601, 701, 601, 701, 601, 701, 601, 701, 601, 701, 601, 703],
}}
TUNED = {size: {key: [run // 100 for run in runs for _ in range(run % 100)] for key, runs in found.items()} for size, found in TUNED.items()}


def plan(n, C):
    if (n, C) in TUNED:
        return TUNED[n, C], PREFIX[n, C]
    table = {}
    for t in range(n):
        w = n - 1 - t
        ops = [(-2, SPREAD), (-1, PAIR)]
        up = {(b, c): b * C + c + LAG * t for b in range(min(t + 1, n - 1)) for c in range(C)}
        down = {(b, c): (b - t) * C + c + LAG * w for b in range(max(t, 1), n) for c in range(C)}
        ops += [(k, UP) for k in up.values()] + [(k, DOWN) for k in down.values()]
        base = n * C + LAG * n
        ops += [(base, MM_UP)] * (t * C // 2) + [(base, MM_DOWN)] * ((n - t) * C // 2)
        ops += [(base, ATTEND)] * (2 * n)
        ops += [(base + 1 + (b - 1) * C + c + 2 * t, SUM_UP) for b in range(t + 1, n) for c in range(C)]
        ops += [(base + 1 + b * C + c + 2 * w, SUM_DOWN) for b in range(t) for c in range(C)]
        ops += [(base + n * C + 2 * n, FIN)] * C
        order = [op for _, op in sorted(ops)]
        for i in range(POLICY_OPS):
            order.insert(len(order) * (i + 1) // (POLICY_OPS + 1), POLICY)
        table[t, 0] = table[t, 1] = order
    return table, [0] * n


def kernel(
    n, R, kvw, heads,
    resid_h, gain, wq_h, wkv_h, wo_h, head, lens, pol_in,
    out_h, rew, pol_out,
    wq, wkv, wo, resid, nrm, part, accq, acckv, kf, vf, att, score, rmy, rin,
    load_sem, send_sem, ag_recv, rs_recv, w_load, w_send, w_recv, r_send, r_recv, p_send, p_recv, p_loc, out_sem,
):
    t = lax.axis_index("tp")
    r = lax.axis_index("rep")
    par = lax.rem(r, 2)
    C = nrm.shape[1]
    rows, cols = nrm.shape[2], nrm.shape[3]
    seq = n * rows
    length = lens[0]
    qw = att.shape[2]

    def chunk_of(ref, c):
        return ref.at[:, pl.ds(pl.multiple_of(c * cols, cols), cols)]

    loads = [pltpu.make_async_copy(chunk_of(resid_h.at[0], c), resid.at[c], load_sem.at[c]) for c in range(C)]
    wload = pltpu.make_async_copy(wq_h, wq, load_sem.at[C])
    oloads = [pltpu.make_async_copy(chunk_of(wo_h, c), wo.at[c], load_sem.at[C + 2 + c]) for c in range(C)]
    for cp in loads:
        cp.start()

    barrier = pltpu.get_barrier_semaphore()
    for k in range(1, n):
        pl.semaphore_signal(barrier, inc=1, device_id={"tp": lax.rem(t + k, n)}, device_id_type=MESH)
    for k in range(1, R):
        pl.semaphore_signal(barrier, inc=1, device_id={"rep": lax.rem(r + k, R)}, device_id_type=MESH)

    pieces = kvw // HS
    group = QH // KVH
    wrows = wkv.shape[0] // R

    def head_of(tp):
        return (tp * heads) // group

    def source(is_v, tp):
        gid = is_v * KVH + head_of(tp)
        return gid // pieces, lax.rem(gid, pieces)

    def wpart(ref, part, col):
        return ref.at[pl.ds(pl.multiple_of(part * wrows, wrows), wrows), pl.ds(pl.multiple_of(col * HS, HS), HS)]

    def w_own(is_v):
        _, p = source(is_v, t)
        return pltpu.make_async_copy(
            wkv_h.at[:, pl.ds(pl.multiple_of(p * HS, HS), HS)], wkv.at[:, is_v * HS : (is_v + 1) * HS], w_load.at[is_v]
        )

    def w_give(is_v, k):
        target = lax.rem(t + k, n)
        owner, p = source(is_v, target)
        return owner == t, pltpu.make_async_remote_copy(
            wpart(wkv_h, r, p), wpart(wkv, r, is_v), w_send.at[0, is_v, k - 1], w_recv.at[is_v, r],
            device_id={"tp": target}, device_id_type=MESH,
        )

    def w_spread(is_v, k):
        return pltpu.make_async_remote_copy(
            wpart(wkv, r, is_v), wpart(wkv, r, is_v), w_send.at[1, is_v, k - 1], w_recv.at[is_v, r],
            device_id={"rep": lax.rem(r + 2 * k, R)}, device_id_type=MESH,
        )

    def w_pair(is_v, k):
        part = lax.rem(r + 2 * k, R)
        return pltpu.make_async_remote_copy(
            wpart(wkv, part, is_v), wpart(wkv, part, is_v), w_send.at[2, is_v, k], w_recv.at[is_v, part],
            device_id={"rep": r + 1 - 2 * par}, device_id_type=MESH,
        )

    def w_wait(is_v, part):
        pltpu.make_async_copy(wpart(wkv, part, is_v), wpart(wkv, part, is_v), w_recv.at[is_v, part]).wait()

    def foreign(is_v, do):
        owner, _ = source(is_v, t)

        @pl.when(owner != t)
        def _():
            do()

    def spread():
        for is_v in (0, 1):
            def do(is_v=is_v):
                w_wait(is_v, r)
                for k in range(1, R // 2):
                    w_spread(is_v, k).start()
            foreign(is_v, do)

    def pair():
        for is_v in (0, 1):
            def do(is_v=is_v):
                w_pair(is_v, 0).start()
                for k in range(1, R // 2):
                    w_wait(is_v, lax.rem(r + 2 * k, R))
                    w_pair(is_v, k).start()
            foreign(is_v, do)

    def weights_here():
        wload.wait()
        for is_v in (0, 1):
            owner, _ = source(is_v, t)

            @pl.when(owner == t)
            def _(is_v=is_v):
                w_own(is_v).wait()

            def do(is_v=is_v):
                for k in range(R // 2):
                    w_wait(is_v, lax.rem(r + 1 - 2 * par + 2 * k, R))
            foreign(is_v, do)

    def weights_drain():
        for is_v in (0, 1):
            for k in range(1, n):
                mine, cp = w_give(is_v, k)

                @pl.when(mine)
                def _(cp=cp):
                    cp.wait_send()

            def do(is_v=is_v):
                for k in range(1, R // 2):
                    w_spread(is_v, k).wait_send()
                for k in range(R // 2):
                    w_pair(is_v, k).wait_send()
            foreign(is_v, do)

    kf[...] = jnp.zeros_like(kf)
    vf[...] = jnp.zeros_like(vf)
    score[...] = jnp.zeros_like(score)
    for b in range(n):
        accq[b] = jnp.zeros(accq.shape[1:], F32)
        acckv[b] = jnp.zeros(acckv.shape[1:], F32)

    pl.semaphore_wait(barrier, n - 1 + R - 1)
    for is_v in (0, 1):
        for k in range(1, n):
            mine, cp = w_give(is_v, k)

            @pl.when(mine)
            def _(cp=cp):
                cp.start()

    for cp in loads:
        cp.wait()
    for is_v in (0, 1):
        owner, _ = source(is_v, t)

        @pl.when(owner == t)
        def _(is_v=is_v):
            w_own(is_v).start()

    for cp in [wload] + oloads:
        cp.start()

    def sq(c, acc):
        x = resid[c].astype(F32)
        return acc + jnp.sum(x * x, axis=1, keepdims=True)

    ms = lax.fori_loop(0, C, sq, jnp.zeros((rows, 1), F32))
    scale = lax.rsqrt(ms / (C * cols) + 1e-05)

    def norm(c, carry):
        nrm[t, c] = (resid[c].astype(F32) * scale * gain[c].astype(F32)).astype(BF16)
        return carry

    lax.fori_loop(0, C, norm, 0)

    steps = R.bit_length() - 1

    def pol(src, s):
        return pltpu.make_async_remote_copy(
            src, pol_out, p_send.at[s], p_recv, device_id={"rep": r + (R >> (s + 1))}, device_id_type=MESH
        )

    def pol_root():
        @pl.when(r == 0)
        def _():
            for s in range(steps):
                pol(pol_in, s).start()
            pltpu.make_async_copy(pol_in, pol_out, p_loc).start()

    def pol_point(s):
        gap = R >> (s + 1)

        @pl.when(lax.rem(r, 2 * gap) == gap)
        def _():
            pltpu.make_async_copy(pol_out, pol_out, p_recv).wait()
            for q in range(s + 1, steps):
                pol(pol_out, q).start()

    table, prefix = plan(n, C)
    total_ops = max(len(ops) for ops in table.values())
    word_count = -(-total_ops // PER_WORD)

    def packed(ops, i):
        part = (ops + [NOTHING] * (word_count * PER_WORD))[i * PER_WORD : (i + 1) * PER_WORD]
        return sum(op << (4 * q) for q, op in enumerate(part))

    def pick(value):
        keys = list(table)
        out = jnp.int32(value(keys[0]))
        for a, p in keys[1:]:
            out = jnp.where((t == a) & (par == p), jnp.int32(value((a, p))), out)
        return out

    words = [pick(lambda key, i=i: packed(table[key], i)) for i in range(word_count)]
    ahead = pick(lambda key: prefix[key[0]])

    def multiply(b, q):
        x0, x1 = nrm[b, 2 * q], nrm[b, 2 * q + 1]
        w0 = wkv[pl.ds(pl.multiple_of(2 * q * cols, cols), cols), :]
        w1 = wkv[pl.ds(pl.multiple_of((2 * q + 1) * cols, cols), cols), :]
        acckv[b] += jnp.dot(x0, w0, preferred_element_type=F32) + jnp.dot(x1, w1, preferred_element_type=F32)
        accq[b] += jnp.dot(x0, wq[2 * q], preferred_element_type=F32) + jnp.dot(
            x1, wq[2 * q + 1], preferred_element_type=F32
        )

        @pl.when(q == C // 2 - 1)
        def _():
            span = pl.ds(pl.multiple_of(b * rows, rows), rows)
            kf[span, :] = acckv[b, :, :HS].astype(BF16)
            vf[span, :] = acckv[b, :, HS:].astype(BF16)

    def ag_copy(d, b, c, slot):
        return pltpu.make_async_remote_copy(
            nrm.at[b, c], nrm.at[b, c], send_sem.at[d, slot], ag_recv.at[b, c],
            device_id={"tp": t + (1 if d == 0 else -1)}, device_id_type=MESH,
        )

    def ag_step(d, i, sent):
        has = (t < n - 1) if d == 0 else (t > 0)
        if d == 0:
            edge = jnp.where(t == n - 1, 0, ahead)
            low = i - edge
            passing = (low >= 0) & (low < t * C)
            own_c = jnp.where(low < 0, i, i - t * C)
            b = jnp.where(passing, jnp.maximum(low, 0) // C, t)
            c = jnp.where(passing, lax.rem(jnp.maximum(low, 0), C), own_c)
        else:
            b = jnp.maximum(t, 1) + i // C
            c = lax.rem(i, C)

        @pl.when(b != t)
        def _():
            pltpu.make_async_copy(nrm.at[b, c], nrm.at[b, c], ag_recv.at[b, c]).wait()

        @pl.when(has)
        def _():
            @pl.when(sent >= DEPTH)
            def _():
                ag_copy(d, b, c, lax.rem(sent, DEPTH)).wait_send()

            ag_copy(d, b, c, lax.rem(sent, DEPTH)).start()

    def rs_copy(d, b, c, slot):
        dst = b if d == 0 else jnp.where(b == t - 1, n, b)
        return pltpu.make_async_remote_copy(
            part.at[b, c], part.at[dst, c], send_sem.at[d, slot], rs_recv.at[dst, c],
            device_id={"tp": t + (1 if d == 0 else -1)}, device_id_type=MESH,
        )

    def rs_wait(slot, c):
        pltpu.make_async_copy(part.at[slot, c], part.at[slot, c], rs_recv.at[slot, c]).wait()

    def project(b, c):
        return jnp.dot(att[b], wo[c], preferred_element_type=F32).astype(BF16)

    def rs_step(d, i, sent):
        b = (t + 1 if d == 0 else 0) + i // C
        c = lax.rem(i, C)
        has = (t > 0) if d == 0 else (t < n - 1)
        mine = project(b, c)

        @pl.when(has)
        def _():
            rs_wait(b, c)
            part[b, c] = (part[b, c].astype(F32) + mine.astype(F32)).astype(BF16)

        @pl.when(jnp.logical_not(has))
        def _():
            part[b, c] = mine

        @pl.when(sent >= DEPTH)
        def _():
            rs_copy(d, b, c, lax.rem(sent, DEPTH)).wait_send()

        rs_copy(d, b, c, lax.rem(sent, DEPTH)).start()

    def attend(b, part_of):
        rowpos = b * rows + lax.broadcasted_iota(jnp.int32, (rows, seq), 0)
        colpos = lax.broadcasted_iota(jnp.int32, (rows, seq), 1)
        valid = (colpos <= rowpos) & (colpos < length)
        wide = qw // 2
        here = pl.ds(pl.multiple_of(part_of * wide, wide), wide)
        q = accq[b, :, here].astype(BF16)
        outs = []
        for h in range(heads // 2):
            s = lax.dot_general(
                q[:, h * HS : (h + 1) * HS], kf[...],
                (((1,), (1,)), ((), ())), preferred_element_type=F32,
            ) * HS ** (-0.5)
            s = jnp.where(valid, s, -1e30)
            e = jnp.exp(s - jnp.max(s, axis=1, keepdims=True))
            pr = (e / jnp.sum(e, axis=1, keepdims=True)).astype(BF16)
            outs.append(jnp.dot(pr, vf[...], preferred_element_type=F32).astype(BF16))
        att[b, :, here] = jnp.concatenate(outs, axis=1)

    def fin(c):
        total = project(t, c).astype(F32)

        @pl.when(t > 0)
        def _():
            rs_wait(t, c)

        @pl.when(t < n - 1)
        def _():
            rs_wait(n, c)

        below = jnp.where(t > 0, part[t, c].astype(F32), 0.0)
        above = jnp.where(t < n - 1, part[n, c].astype(F32), 0.0)
        hid = (resid[c].astype(F32) + (total + below + above)).astype(BF16)
        resid[c] = hid
        pltpu.make_async_copy(resid.at[c], chunk_of(out_h.at[0], c), out_sem.at[c]).start()
        weighed = hid.astype(F32) * head[c].astype(F32)
        acc = score[...]
        for q in range(cols // HS):
            acc = acc + weighed[:, q * HS : (q + 1) * HS]
        score[...] = acc


    def policy(i):
        @pl.when(i == 0)
        def _():
            pol_root()

        for s in range(steps - 1):
            @pl.when(i == min(s + 1, POLICY_OPS - 1))
            def _(s=s):
                pol_point(s)

    def one(k, pos):
        word = words[0]
        for i in range(1, word_count):
            word = jnp.where(k // PER_WORD == i, words[i], word)
        op = lax.rem(lax.shift_right_logical(word, 4 * lax.rem(k, PER_WORD)), 16)

        def at(kind, do):
            @pl.when(op == kind)
            def _():
                do(pos[kind])

        half = C // 2
        at(UP, lambda i: ag_step(0, i, i + pos[SUM_UP]))
        at(DOWN, lambda i: ag_step(1, i, i + pos[SUM_DOWN]))

        @pl.when((op == MM_UP) | (op == MM_DOWN))
        def _():
            first = pos[MM_UP] + pos[MM_DOWN] == 0

            @pl.when(first)
            def _():
                weights_here()

            i = jnp.where(op == MM_UP, pos[MM_UP], pos[MM_DOWN] + t * half)
            multiply(i // half, lax.rem(i, half))

        at(ATTEND, lambda i: attend(i // 2, lax.rem(i, 2)))

        @pl.when((op == SUM_UP) | (op == SUM_DOWN) | (op == FIN))
        def _():
            @pl.when(pos[SUM_UP] + pos[SUM_DOWN] + pos[FIN] == 0)
            def _():
                for cp in oloads:
                    cp.wait()

        at(SUM_UP, lambda i: rs_step(0, i, i + pos[UP]))
        at(SUM_DOWN, lambda i: rs_step(1, i, i + pos[DOWN]))
        at(FIN, fin)
        at(SPREAD, lambda i: spread())
        at(PAIR, lambda i: pair())
        at(POLICY, policy)
        return tuple(p + jnp.where(op == kind, 1, 0) for kind, p in enumerate(pos))

    lax.fori_loop(0, total_ops, one, (jnp.int32(0),) * 11)

    local_last = length - 1 - t * rows
    rowid = lax.broadcasted_iota(jnp.int32, (rows, 1), 0)
    weight = jnp.where(rowid == local_last, 1.0, 0.0) + seq ** (-0.5)
    rmy[...] = jnp.broadcast_to(jnp.sum(score[...] * weight, keepdims=True), rmy.shape)

    def rcopy(k):
        return pltpu.make_async_remote_copy(
            rmy, rin.at[k - 1], r_send.at[k - 1], r_recv.at[k - 1],
            device_id={"tp": lax.rem(t + k, n)}, device_id_type=MESH,
        )

    for k in range(1, n):
        rcopy(k).start()
    pol_point(steps - 1)

    for d in (0, 1):
        has = (t < n - 1) if d == 0 else (t > 0)

        @pl.when(has)
        def _(d=d):
            for q in range(DEPTH):
                ag_copy(d, t, 0, q).wait_send()

    weights_drain()

    total = rmy[...]
    for k in range(1, n):
        rcopy(k).wait()
        total = total + rin[k - 1]
    rew[...] = total
    for c in range(C):
        pltpu.make_async_copy(resid.at[c], chunk_of(out_h.at[0], c), out_sem.at[c]).wait()

    @pl.when(r == 0)
    def _():
        for s in range(steps):
            pol(pol_in, s).wait_send()
        pltpu.make_async_copy(pol_in, pol_out, p_loc).wait()

    for s in range(steps - 1):
        gap = R >> (s + 1)

        @pl.when(lax.rem(r, 2 * gap) == gap)
        def _(s=s):
            for q in range(s + 1, steps):
                pol(pol_out, q).wait_send()


def solution(mesh):
    n, R = mesh.shape["tp"], mesh.shape["rep"]

    def on_device(residual_in, norm_gain, w_query, w_keyval, w_out, score_head, lengths, policy_slots):
        rows, width = residual_in.shape[1:]
        qw, kvw = w_query.shape[1], w_keyval.shape[1]
        heads = qw // HS
        C = CHUNKS
        cols = width // C
        sem = pltpu.SemaphoreType.DMA
        vm = pl.BlockSpec(memory_space=pltpu.VMEM)
        hbm = pl.BlockSpec(memory_space=pl.ANY)
        hidden, reward, policy = pl.pallas_call(
            functools.partial(kernel, n, R, kvw, heads),
            out_shape=(
                jax.ShapeDtypeStruct(residual_in.shape, BF16),
                jax.ShapeDtypeStruct((8, 128), F32),
                jax.ShapeDtypeStruct(policy_slots.shape, BF16),
            ),
            in_specs=[hbm, vm, hbm, hbm, hbm, vm, pl.BlockSpec(memory_space=pltpu.SMEM), hbm],
            out_specs=(hbm, vm, hbm),
            scratch_shapes=[
                pltpu.VMEM((C, cols, qw), BF16),
                pltpu.VMEM((width, 2 * HS), BF16),
                pltpu.VMEM((C, qw, cols), BF16),
                pltpu.VMEM((C, rows, cols), BF16),
                pltpu.VMEM((n, C, rows, cols), BF16),
                pltpu.VMEM((n + 1, C, rows, cols), BF16),
                pltpu.VMEM((n, rows, qw), F32),
                pltpu.VMEM((n, rows, 2 * HS), F32),
                pltpu.VMEM((n * rows, HS), BF16),
                pltpu.VMEM((n * rows, HS), BF16),
                pltpu.VMEM((n, rows, qw), BF16),
                pltpu.VMEM((rows, 128), F32),
                pltpu.VMEM((8, 128), F32),
                pltpu.VMEM((n - 1, 8, 128), F32),
                sem((2 * C + 2,)),
                sem((2, DEPTH)),
                sem((n, C)),
                sem((n + 1, C)),
                sem((2,)),
                sem((3, 2, max(n, R // 2))),
                sem((2, R)),
                sem((n - 1,)),
                sem((n - 1,)),
                sem((R.bit_length() - 1,)),
                sem,
                sem,
                sem((C,)),
            ],
            compiler_params=pltpu.CompilerParams(
                collective_id=0, has_side_effects=True, vmem_limit_bytes=67043328
            ),
        )(
            residual_in,
            norm_gain.reshape(C, 1, cols),
            w_query.reshape(C, cols, qw),
            w_keyval,
            w_out,
            score_head.reshape(C, 1, cols),
            lengths,
            policy_slots,
        )
        return hidden, reward[0, :1], policy

    return jax.shard_map(
        on_device,
        mesh=mesh,
        in_specs=(
            P("rep", "tp", None),
            P(),
            P(None, "tp"),
            P(None, "tp"),
            P("tp", None),
            P(),
            P("rep"),
            P("rep", None, "tp"),
        ),
        out_specs=(P("rep", "tp", None), P("rep"), P("rep", None, "tp")),
        check_vma=False,
    )
```

```python
import functools

import jax
import jax.numpy as jnp
from jax import lax
from jax.experimental import pallas as pl
from jax.experimental.pallas import tpu as pltpu
from jax.sharding import PartitionSpec as P

QH = 32
KVH = 4
HS = 128
MESH = pl.DeviceIdType.MESH
F32 = jnp.float32
BF16 = jnp.bfloat16
CHUNKS = 8
DEPTH = 2
LAG = 2
NEVER = 1 << 20
UP, DOWN, MM_UP, MM_DOWN, ATTEND, SUM_UP, SUM_DOWN, FIN, SPREAD, PAIR, POLICY = range(11)
NOTHING = 15
PER_WORD = 7
POLICY_OPS = 4

PREFIX = {(4, 8): [0, 0, 1, 0]}
GATE = {(4, 8): ([7, 6, 6, 29], [29, 5, 16, 2])}
TUNED = {(4, 8): {
    (0, 0): [3, 101, 2, 101, 1, 801, 1, 101, 1, 102, 901, 303, 1001, 301, 402, 302, 101, 301, 102, 301, 402, 502, 102, 301, 501, 101, 501, 101, 501, 301, 501, 101, 501, 1001, 501, 101, 301, 102, 301, 402, 502, 102, 501, 301, 501, 101, 502, 101, 501, 301, 501, 102, 301, 102, 1001, 301, 402, 502, 702, 502, 1001, 701, 502, 701, 502, 704],
    (0, 1): [801, 3, 101, 901, 1, 101, 1, 301, 101, 301, 1, 301, 1, 301, 101, 1, 1001, 302, 401, 101, 401, 101, 301, 102, 301, 402, 502, 102, 301, 502, 101, 501, 101, 301, 502, 101, 1001, 501, 101, 301, 102, 301, 402, 101, 502, 101, 301, 501, 101, 502, 101, 301, 502, 101, 501, 101, 301, 102, 1001, 301, 402, 502, 702, 501, 701, 1001, 502, 701, 502, 701, 501, 703],
    (1, 0): [103, 1, 101, 1, 801, 1, 101, 2, 101, 1, 101, 1, 101, 2, 101, 1001, 901, 1, 101, 302, 1, 303, 1, 102, 301, 1, 202, 101, 201, 1, 201, 401, 1, 402, 1, 401, 101, 301, 101, 1001, 101, 301, 402, 102, 301, 102, 301, 501, 101, 502, 101, 301, 502, 101, 701, 501, 101, 501, 301, 401, 501, 401, 601, 701, 601, 1001, 702, 601, 701, 601, 701, 501, 601, 701, 1001, 501, 601, 501, 701, 501, 601, 502, 601, 502],
    (1, 1): [801, 103, 1, 101, 1, 101, 1, 901, 101, 2, 301, 101, 303, 101, 1001, 202, 1, 201, 2, 201, 401, 101, 401, 101, 301, 402, 101, 2, 101, 301, 2, 101, 2, 101, 301, 2, 101, 1001, 101, 301, 402, 102, 301, 102, 301, 101, 501, 101, 301, 502, 101, 502, 101, 301, 502, 401, 601, 501, 401, 603, 1001, 601, 501, 701, 501, 601, 701, 501, 701, 501, 1001, 601, 701, 501, 701, 501, 601, 701, 501, 701, 501, 701],
    (2, 0): [1, 103, 801, 1, 101, 1, 101, 1, 101, 1, 101, 1, 102, 1, 102, 1001, 1, 101, 901, 102, 1, 204, 1, 101, 401, 1, 201, 101, 401, 1, 302, 601, 1, 201, 601, 301, 1, 301, 601, 301, 1001, 301, 601, 1, 201, 1, 301, 601, 301, 1, 201, 601, 1, 402, 601, 1, 402, 601, 1, 402, 2, 601, 1, 601, 1, 602, 1001, 604, 703, 502, 1001, 701, 502, 701, 502, 701, 501, 701, 501, 701],
    (2, 1): [801, 2, 901, 1, 201, 1, 303, 1, 201, 301, 1, 103, 1, 201, 1001, 101, 1, 101, 1, 201, 101, 402, 101, 2, 201, 101, 1, 101, 1, 201, 101, 301, 1, 101, 1, 201, 101, 301, 1, 101, 1, 201, 1001, 101, 402, 101, 402, 101, 2, 302, 402, 2, 602, 2, 601, 1, 609, 1001, 601, 501, 602, 501, 601, 501, 701, 501, 1001, 701, 501, 701, 501, 701, 501, 701, 501, 703],
    (3, 0): [103, 801, 101, 1, 101, 2, 101, 901, 1, 202, 304, 1001, 2, 201, 1, 102, 1, 201, 402, 602, 1, 602, 1, 601, 201, 601, 1, 602, 1, 201, 2, 1001, 201, 2, 201, 402, 602, 2, 201, 1, 601, 1, 201, 601, 1, 601, 1, 201, 602, 1, 601, 1, 201, 401, 1001, 401, 602, 402, 604, 1001, 701, 601, 702, 601, 705],
    (3, 1): [103, 801, 103, 901, 101, 304, 101, 2, 201, 1, 1001, 1, 201, 2, 201, 2, 201, 402, 602, 1, 601, 1, 601, 201, 601, 1, 602, 1, 201, 601, 2, 1001, 201, 2, 201, 402, 602, 2, 201, 1, 601, 1, 201, 1, 601, 1, 201, 1, 601, 1, 201, 401, 601, 402, 1001, 601, 401, 604, 701, 602, 1001, 701, 601, 701, 601, 701, 601, 704],
}}
TUNED = {size: {key: [run // 100 for run in runs for _ in range(run % 100)] for key, runs in found.items()} for size, found in TUNED.items()}


def plan(n, C):
    if (n, C) in TUNED:
        return TUNED[n, C], PREFIX[n, C], GATE[n, C]
    table = {}
    for t in range(n):
        w = n - 1 - t
        ops = [(-2, SPREAD), (-1, PAIR)]
        up = {(b, c): b * C + c + LAG * t for b in range(min(t + 1, n - 1)) for c in range(C)}
        down = {(b, c): (b - t) * C + c + LAG * w for b in range(max(t, 1), n) for c in range(C)}
        ops += [(k, UP) for k in up.values()] + [(k, DOWN) for k in down.values()]
        base = n * C + LAG * n
        ops += [(base, MM_UP)] * (t * C // 2) + [(base, MM_DOWN)] * ((n - t) * C // 2)
        ops += [(base, ATTEND)] * (2 * n)
        ops += [(base + 1 + (b - 1) * C + c + 2 * t, SUM_UP) for b in range(t + 1, n) for c in range(C)]
        ops += [(base + 1 + b * C + c + 2 * w, SUM_DOWN) for b in range(t) for c in range(C)]
        ops += [(base + n * C + 2 * n, FIN)] * C
        order = [op for _, op in sorted(ops)]
        for i in range(POLICY_OPS):
            order.insert(len(order) * (i + 1) // (POLICY_OPS + 1), POLICY)
        table[t, 0] = table[t, 1] = order
    return table, [0] * n, ([1] * n, [1] * n)


def kernel(
    n, R, kvw, heads,
    resid_h, gain, wq_h, wkv_h, wo_h, head, lens, pol_in,
    out_h, rew, pol_out,
    wq, wkv, wo, resid, nrm, part, accq, acckv, kf, vf, att, score, rmy, rin,
    load_sem, send_sem, ag_recv, rs_recv, w_load, w_send, w_recv, r_send, r_recv, p_send, p_recv, p_loc, out_sem, go_sem,
):
    t = lax.axis_index("tp")
    r = lax.axis_index("rep")
    par = lax.rem(r, 2)
    C = nrm.shape[1]
    rows, cols = nrm.shape[2], nrm.shape[3]
    seq = n * rows
    length = lens[0]
    qw = att.shape[2]

    def chunk_of(ref, c):
        return ref.at[:, pl.ds(pl.multiple_of(c * cols, cols), cols)]

    loads = [pltpu.make_async_copy(chunk_of(resid_h.at[0], c), resid.at[c], load_sem.at[c]) for c in range(C)]
    wload = pltpu.make_async_copy(wq_h, wq, load_sem.at[C])
    oloads = [pltpu.make_async_copy(chunk_of(wo_h, c), wo.at[c], load_sem.at[C + 2 + c]) for c in range(C)]
    for cp in loads:
        cp.start()

    barrier = pltpu.get_barrier_semaphore()
    for k in range(1, n):
        pl.semaphore_signal(barrier, inc=1, device_id={"tp": lax.rem(t + k, n)}, device_id_type=MESH)
    for k in range(1, R):
        pl.semaphore_signal(barrier, inc=1, device_id={"rep": lax.rem(r + k, R)}, device_id_type=MESH)

    pieces = kvw // HS
    group = QH // KVH
    wrows = wkv.shape[0] // R

    def head_of(tp):
        return (tp * heads) // group

    def source(is_v, tp):
        gid = is_v * KVH + head_of(tp)
        return gid // pieces, lax.rem(gid, pieces)

    def wpart(ref, part, col):
        return ref.at[pl.ds(pl.multiple_of(part * wrows, wrows), wrows), pl.ds(pl.multiple_of(col * HS, HS), HS)]

    def w_own(is_v):
        _, p = source(is_v, t)
        return pltpu.make_async_copy(
            wkv_h.at[:, pl.ds(pl.multiple_of(p * HS, HS), HS)], wkv.at[:, is_v * HS : (is_v + 1) * HS], w_load.at[is_v]
        )

    def w_give(is_v, k):
        target = lax.rem(t + k, n)
        owner, p = source(is_v, target)
        return owner == t, pltpu.make_async_remote_copy(
            wpart(wkv_h, r, p), wpart(wkv, r, is_v), w_send.at[0, is_v, k - 1], w_recv.at[is_v, r],
            device_id={"tp": target}, device_id_type=MESH,
        )

    def w_spread(is_v, k):
        return pltpu.make_async_remote_copy(
            wpart(wkv, r, is_v), wpart(wkv, r, is_v), w_send.at[1, is_v, k - 1], w_recv.at[is_v, r],
            device_id={"rep": lax.rem(r + 2 * k, R)}, device_id_type=MESH,
        )

    def w_pair(is_v, k):
        part = lax.rem(r + 2 * k, R)
        return pltpu.make_async_remote_copy(
            wpart(wkv, part, is_v), wpart(wkv, part, is_v), w_send.at[2, is_v, k], w_recv.at[is_v, part],
            device_id={"rep": r + 1 - 2 * par}, device_id_type=MESH,
        )

    def w_wait(is_v, part):
        pltpu.make_async_copy(wpart(wkv, part, is_v), wpart(wkv, part, is_v), w_recv.at[is_v, part]).wait()

    def foreign(is_v, do):
        owner, _ = source(is_v, t)

        @pl.when(owner != t)
        def _():
            do()

    def spread():
        for is_v in (0, 1):
            def do(is_v=is_v):
                w_wait(is_v, r)
                for k in range(1, R // 2):
                    w_spread(is_v, k).start()
            foreign(is_v, do)

    def pair():
        for is_v in (0, 1):
            def do(is_v=is_v):
                w_pair(is_v, 0).start()
                for k in range(1, R // 2):
                    w_wait(is_v, lax.rem(r + 2 * k, R))
                    w_pair(is_v, k).start()
            foreign(is_v, do)

    def weights_here():
        wload.wait()
        for is_v in (0, 1):
            owner, _ = source(is_v, t)

            @pl.when(owner == t)
            def _(is_v=is_v):
                w_own(is_v).wait()

            def do(is_v=is_v):
                for k in range(R // 2):
                    w_wait(is_v, lax.rem(r + 1 - 2 * par + 2 * k, R))
            foreign(is_v, do)

    def weights_drain():
        for is_v in (0, 1):
            for k in range(1, n):
                mine, cp = w_give(is_v, k)

                @pl.when(mine)
                def _(cp=cp):
                    cp.wait_send()

            def do(is_v=is_v):
                for k in range(1, R // 2):
                    w_spread(is_v, k).wait_send()
                for k in range(R // 2):
                    w_pair(is_v, k).wait_send()
            foreign(is_v, do)

    kf[...] = jnp.zeros_like(kf)
    vf[...] = jnp.zeros_like(vf)
    score[...] = jnp.zeros_like(score)
    for b in range(n):
        accq[b] = jnp.zeros(accq.shape[1:], F32)
        acckv[b] = jnp.zeros(acckv.shape[1:], F32)

    pl.semaphore_wait(barrier, n - 1 + R - 1)
    for is_v in (0, 1):
        for k in range(1, n):
            mine, cp = w_give(is_v, k)

            @pl.when(mine)
            def _(cp=cp):
                cp.start()

    for cp in loads:
        cp.wait()
    for is_v in (0, 1):
        owner, _ = source(is_v, t)

        @pl.when(owner == t)
        def _(is_v=is_v):
            w_own(is_v).start()

    for cp in [wload] + oloads:
        cp.start()

    def sq(c, acc):
        x = resid[c].astype(F32)
        return acc + jnp.sum(x * x, axis=1, keepdims=True)

    ms = lax.fori_loop(0, C, sq, jnp.zeros((rows, 1), F32))
    scale = lax.rsqrt(ms / (C * cols) + 1e-05)

    def norm(c, carry):
        nrm[t, c] = (resid[c].astype(F32) * scale * gain[c].astype(F32)).astype(BF16)
        return carry

    lax.fori_loop(0, C, norm, 0)

    steps = R.bit_length() - 1

    def pol(src, s):
        return pltpu.make_async_remote_copy(
            src, pol_out, p_send.at[s], p_recv, device_id={"rep": r + (R >> (s + 1))}, device_id_type=MESH
        )

    def pol_root():
        @pl.when(r == 0)
        def _():
            for s in range(steps):
                pol(pol_in, s).start()
            pltpu.make_async_copy(pol_in, pol_out, p_loc).start()

    def pol_point(s):
        gap = R >> (s + 1)

        @pl.when(lax.rem(r, 2 * gap) == gap)
        def _():
            pltpu.make_async_copy(pol_out, pol_out, p_recv).wait()
            for q in range(s + 1, steps):
                pol(pol_out, q).start()

    table, prefix, gate = plan(n, C)
    total_ops = max(len(ops) for ops in table.values())
    word_count = -(-total_ops // PER_WORD)

    def packed(ops, i):
        part = (ops + [NOTHING] * (word_count * PER_WORD))[i * PER_WORD : (i + 1) * PER_WORD]
        return sum(op << (4 * q) for q, op in enumerate(part))

    def pick(value):
        keys = list(table)
        out = jnp.int32(value(keys[0]))
        for a, p in keys[1:]:
            out = jnp.where((t == a) & (par == p), jnp.int32(value((a, p))), out)
        return out

    words = [pick(lambda key, i=i: packed(table[key], i)) for i in range(word_count)]
    ahead = pick(lambda key: prefix[key[0]])
    release = [pick(lambda key, d=d: gate[d][key[0]]) for d in (0, 1)]

    def multiply(b, q):
        x0, x1 = nrm[b, 2 * q], nrm[b, 2 * q + 1]
        w0 = wkv[pl.ds(pl.multiple_of(2 * q * cols, cols), cols), :]
        w1 = wkv[pl.ds(pl.multiple_of((2 * q + 1) * cols, cols), cols), :]
        acckv[b] += jnp.dot(x0, w0, preferred_element_type=F32) + jnp.dot(x1, w1, preferred_element_type=F32)
        accq[b] += jnp.dot(x0, wq[2 * q], preferred_element_type=F32) + jnp.dot(
            x1, wq[2 * q + 1], preferred_element_type=F32
        )

        @pl.when(q == C // 2 - 1)
        def _():
            span = pl.ds(pl.multiple_of(b * rows, rows), rows)
            kf[span, :] = acckv[b, :, :HS].astype(BF16)
            vf[span, :] = acckv[b, :, HS:].astype(BF16)

    def ag_copy(d, b, c, slot):
        return pltpu.make_async_remote_copy(
            nrm.at[b, c], nrm.at[b, c], send_sem.at[d, slot], ag_recv.at[b, c],
            device_id={"tp": t + (1 if d == 0 else -1)}, device_id_type=MESH,
        )

    def ag_step(d, i, sent):
        has = (t < n - 1) if d == 0 else (t > 0)
        if d == 0:
            edge = jnp.where(t == n - 1, 0, ahead)
            low = i - edge
            passing = (low >= 0) & (low < t * C)
            own_c = jnp.where(low < 0, i, i - t * C)
            b = jnp.where(passing, jnp.maximum(low, 0) // C, t)
            c = jnp.where(passing, lax.rem(jnp.maximum(low, 0), C), own_c)
        else:
            b = jnp.maximum(t, 1) + i // C
            c = lax.rem(i, C)

        @pl.when(b != t)
        def _():
            pltpu.make_async_copy(nrm.at[b, c], nrm.at[b, c], ag_recv.at[b, c]).wait()

        @pl.when(has & (par == 1) & (i == 0))
        def _():
            pl.semaphore_wait(go_sem.at[d], 1)

        @pl.when(has)
        def _():
            @pl.when(sent >= DEPTH)
            def _():
                ag_copy(d, b, c, lax.rem(sent, DEPTH)).wait_send()

            ag_copy(d, b, c, lax.rem(sent, DEPTH)).start()

        @pl.when(has & (par == 0) & (i + 1 == release[d]))
        def _():
            pl.semaphore_signal(go_sem.at[d], inc=1, device_id={"rep": r + 1}, device_id_type=MESH)

    def rs_copy(d, b, c, slot):
        dst = b if d == 0 else jnp.where(b == t - 1, n, b)
        return pltpu.make_async_remote_copy(
            part.at[b, c], part.at[dst, c], send_sem.at[d, slot], rs_recv.at[dst, c],
            device_id={"tp": t + (1 if d == 0 else -1)}, device_id_type=MESH,
        )

    def rs_wait(slot, c):
        pltpu.make_async_copy(part.at[slot, c], part.at[slot, c], rs_recv.at[slot, c]).wait()

    def project(b, c):
        return jnp.dot(att[b], wo[c], preferred_element_type=F32).astype(BF16)

    def rs_step(d, i, sent):
        b = (t + 1 if d == 0 else 0) + i // C
        c = lax.rem(i, C)
        has = (t > 0) if d == 0 else (t < n - 1)
        mine = project(b, c)

        @pl.when(has)
        def _():
            rs_wait(b, c)
            part[b, c] = (part[b, c].astype(F32) + mine.astype(F32)).astype(BF16)

        @pl.when(jnp.logical_not(has))
        def _():
            part[b, c] = mine

        @pl.when(sent >= DEPTH)
        def _():
            rs_copy(d, b, c, lax.rem(sent, DEPTH)).wait_send()

        rs_copy(d, b, c, lax.rem(sent, DEPTH)).start()

    def attend(b, part_of):
        rowpos = b * rows + lax.broadcasted_iota(jnp.int32, (rows, seq), 0)
        colpos = lax.broadcasted_iota(jnp.int32, (rows, seq), 1)
        valid = (colpos <= rowpos) & (colpos < length)
        wide = qw // 2
        here = pl.ds(pl.multiple_of(part_of * wide, wide), wide)
        q = accq[b, :, here].astype(BF16)
        outs = []
        for h in range(heads // 2):
            s = lax.dot_general(
                q[:, h * HS : (h + 1) * HS], kf[...],
                (((1,), (1,)), ((), ())), preferred_element_type=F32,
            ) * HS ** (-0.5)
            s = jnp.where(valid, s, -1e30)
            e = jnp.exp(s - jnp.max(s, axis=1, keepdims=True))
            pr = (e / jnp.sum(e, axis=1, keepdims=True)).astype(BF16)
            outs.append(jnp.dot(pr, vf[...], preferred_element_type=F32).astype(BF16))
        att[b, :, here] = jnp.concatenate(outs, axis=1)

    def fin(c):
        total = project(t, c).astype(F32)

        @pl.when(t > 0)
        def _():
            rs_wait(t, c)

        @pl.when(t < n - 1)
        def _():
            rs_wait(n, c)

        below = jnp.where(t > 0, part[t, c].astype(F32), 0.0)
        above = jnp.where(t < n - 1, part[n, c].astype(F32), 0.0)
        hid = (resid[c].astype(F32) + (total + below + above)).astype(BF16)
        resid[c] = hid
        pltpu.make_async_copy(resid.at[c], chunk_of(out_h.at[0], c), out_sem.at[c]).start()
        weighed = hid.astype(F32) * head[c].astype(F32)
        acc = score[...]
        for q in range(cols // HS):
            acc = acc + weighed[:, q * HS : (q + 1) * HS]
        score[...] = acc


    def policy(i):
        @pl.when(i == 0)
        def _():
            pol_root()

        for s in range(steps - 1):
            @pl.when(i == min(s + 1, POLICY_OPS - 1))
            def _(s=s):
                pol_point(s)

    def one(k, pos):
        word = words[0]
        for i in range(1, word_count):
            word = jnp.where(k // PER_WORD == i, words[i], word)
        op = lax.rem(lax.shift_right_logical(word, 4 * lax.rem(k, PER_WORD)), 16)

        def at(kind, do):
            @pl.when(op == kind)
            def _():
                do(pos[kind])

        half = C // 2
        at(UP, lambda i: ag_step(0, i, i + pos[SUM_UP]))
        at(DOWN, lambda i: ag_step(1, i, i + pos[SUM_DOWN]))

        @pl.when((op == MM_UP) | (op == MM_DOWN))
        def _():
            first = pos[MM_UP] + pos[MM_DOWN] == 0

            @pl.when(first)
            def _():
                weights_here()

            i = jnp.where(op == MM_UP, pos[MM_UP], pos[MM_DOWN] + t * half)
            multiply(i // half, lax.rem(i, half))

        at(ATTEND, lambda i: attend(i // 2, lax.rem(i, 2)))

        @pl.when((op == SUM_UP) | (op == SUM_DOWN) | (op == FIN))
        def _():
            @pl.when(pos[SUM_UP] + pos[SUM_DOWN] + pos[FIN] == 0)
            def _():
                for cp in oloads:
                    cp.wait()

        at(SUM_UP, lambda i: rs_step(0, i, i + pos[UP]))
        at(SUM_DOWN, lambda i: rs_step(1, i, i + pos[DOWN]))
        at(FIN, fin)
        at(SPREAD, lambda i: spread())
        at(PAIR, lambda i: pair())
        at(POLICY, policy)
        return tuple(p + jnp.where(op == kind, 1, 0) for kind, p in enumerate(pos))

    lax.fori_loop(0, total_ops, one, (jnp.int32(0),) * 11)

    local_last = length - 1 - t * rows
    rowid = lax.broadcasted_iota(jnp.int32, (rows, 1), 0)
    weight = jnp.where(rowid == local_last, 1.0, 0.0) + seq ** (-0.5)
    rmy[...] = jnp.broadcast_to(jnp.sum(score[...] * weight, keepdims=True), rmy.shape)

    def rcopy(k):
        return pltpu.make_async_remote_copy(
            rmy, rin.at[k - 1], r_send.at[k - 1], r_recv.at[k - 1],
            device_id={"tp": lax.rem(t + k, n)}, device_id_type=MESH,
        )

    for k in range(1, n):
        rcopy(k).start()
    pol_point(steps - 1)

    for d in (0, 1):
        has = (t < n - 1) if d == 0 else (t > 0)

        @pl.when(has)
        def _(d=d):
            for q in range(DEPTH):
                ag_copy(d, t, 0, q).wait_send()

    weights_drain()

    total = rmy[...]
    for k in range(1, n):
        rcopy(k).wait()
        total = total + rin[k - 1]
    rew[...] = total
    for c in range(C):
        pltpu.make_async_copy(resid.at[c], chunk_of(out_h.at[0], c), out_sem.at[c]).wait()

    @pl.when(r == 0)
    def _():
        for s in range(steps):
            pol(pol_in, s).wait_send()
        pltpu.make_async_copy(pol_in, pol_out, p_loc).wait()

    for s in range(steps - 1):
        gap = R >> (s + 1)

        @pl.when(lax.rem(r, 2 * gap) == gap)
        def _(s=s):
            for q in range(s + 1, steps):
                pol(pol_out, q).wait_send()


def solution(mesh):
    n, R = mesh.shape["tp"], mesh.shape["rep"]

    def on_device(residual_in, norm_gain, w_query, w_keyval, w_out, score_head, lengths, policy_slots):
        rows, width = residual_in.shape[1:]
        qw, kvw = w_query.shape[1], w_keyval.shape[1]
        heads = qw // HS
        C = CHUNKS
        cols = width // C
        sem = pltpu.SemaphoreType.DMA
        vm = pl.BlockSpec(memory_space=pltpu.VMEM)
        hbm = pl.BlockSpec(memory_space=pl.ANY)
        hidden, reward, policy = pl.pallas_call(
            functools.partial(kernel, n, R, kvw, heads),
            out_shape=(
                jax.ShapeDtypeStruct(residual_in.shape, BF16),
                jax.ShapeDtypeStruct((8, 128), F32),
                jax.ShapeDtypeStruct(policy_slots.shape, BF16),
            ),
            in_specs=[hbm, vm, hbm, hbm, hbm, vm, pl.BlockSpec(memory_space=pltpu.SMEM), hbm],
            out_specs=(hbm, vm, hbm),
            scratch_shapes=[
                pltpu.VMEM((C, cols, qw), BF16),
                pltpu.VMEM((width, 2 * HS), BF16),
                pltpu.VMEM((C, qw, cols), BF16),
                pltpu.VMEM((C, rows, cols), BF16),
                pltpu.VMEM((n, C, rows, cols), BF16),
                pltpu.VMEM((n + 1, C, rows, cols), BF16),
                pltpu.VMEM((n, rows, qw), F32),
                pltpu.VMEM((n, rows, 2 * HS), F32),
                pltpu.VMEM((n * rows, HS), BF16),
                pltpu.VMEM((n * rows, HS), BF16),
                pltpu.VMEM((n, rows, qw), BF16),
                pltpu.VMEM((rows, 128), F32),
                pltpu.VMEM((8, 128), F32),
                pltpu.VMEM((n - 1, 8, 128), F32),
                sem((2 * C + 2,)),
                sem((2, DEPTH)),
                sem((n, C)),
                sem((n + 1, C)),
                sem((2,)),
                sem((3, 2, max(n, R // 2))),
                sem((2, R)),
                sem((n - 1,)),
                sem((n - 1,)),
                sem((R.bit_length() - 1,)),
                sem,
                sem,
                sem((C,)),
                pltpu.SemaphoreType.REGULAR((2,)),
            ],
            compiler_params=pltpu.CompilerParams(
                collective_id=0, has_side_effects=True, vmem_limit_bytes=67043328
            ),
        )(
            residual_in,
            norm_gain.reshape(C, 1, cols),
            w_query.reshape(C, cols, qw),
            w_keyval,
            w_out,
            score_head.reshape(C, 1, cols),
            lengths,
            policy_slots,
        )
        return hidden, reward[0, :1], policy

    return jax.shard_map(
        on_device,
        mesh=mesh,
        in_specs=(
            P("rep", "tp", None),
            P(),
            P(None, "tp"),
            P(None, "tp"),
            P("tp", None),
            P(),
            P("rep"),
            P("rep", None, "tp"),
        ),
        out_specs=(P("rep", "tp", None), P("rep"), P("rep", None, "tp")),
        check_vma=False,
    )
```
